8 devices in a mesh: dp: 2 (over y, z), tp: 4 (over x, core).
Axes of the slice: x: 2, y: 2, z: 1, core: 2. Of those that a mesh axis runs over, the one named last changes fastest.
Arguments:
- x: bfloat16 [4096, 6656], P('dp'), parts along dimension 0
- gain: bfloat16 [6656], replicated
- wq: bfloat16 [6656, 6656], P(None, 'tp')
- wk: bfloat16 [6656, 6656], P(None, 'tp')
- wv: bfloat16 [6656, 6656], P(None, 'tp')
- wo: bfloat16 [6656, 6656], P('tp')
Outputs:
- output: bfloat16 [4096, 6656], P('dp'), parts along dimension 0
There are 2 independent parts. The reference program is written for one: setup_inputs(seed, part) draws one part's arguments, and reference() takes and returns one part's arrays. A program takes and returns all parts, laid end to end along the dimension named above; an argument that names none is the same for every part.
All inputs are finite; a program needn't handle non-finite values.
Results may differ from the reference program's by a relative error of at most 0.012.
Values are sent between devices in bfloat16 or wider.
A program may use at most 2 GiB of HBM per device.

```python
import jax
import jax.numpy as jnp
from jax import lax

ROWS = 2048
D = 6656
HEADS = 52
KV_HEADS = 52
HEAD = 128
THETA = 10000


def setup_inputs(seed: int = 0, part: int = 0) -> dict:
    kx, kn, kq, kk, kv, ko = jax.random.split(jax.random.key(seed), 6)

    def weights(key, rows, columns):
        return jax.random.normal(key, (rows, columns), jnp.float32) * rows**-0.5

    drawn = {
        "x": jax.random.normal(jax.random.fold_in(kx, part), (ROWS, D), jnp.float32),
        "gain": 1 + 0.1 * jax.random.normal(kn, (D,), jnp.float32),
        "wq": 2 * weights(kq, D, HEADS * HEAD),
        "wk": 2 * weights(kk, D, KV_HEADS * HEAD),
        "wv": 4 * weights(kv, D, KV_HEADS * HEAD),
        "wo": weights(ko, HEADS * HEAD, D),
    }
    return {k: v.astype(jnp.bfloat16) for k, v in drawn.items()}


def normed(x, gain):
    wide = x.astype(jnp.float32)
    scale = lax.rsqrt(jnp.mean(wide * wide, -1, keepdims=True) + 1e-6)
    return (wide * scale * gain.astype(jnp.float32)).astype(jnp.bfloat16)


def turned(t, place, theta):
    half = t.shape[-1] // 2
    angle = place.astype(jnp.float32)[:, None] * theta ** (-jnp.arange(half, dtype=jnp.float32) / half)
    cos, sin = jnp.cos(angle)[:, None], jnp.sin(angle)[:, None]
    a, b = t[..., :half].astype(jnp.float32), t[..., half:].astype(jnp.float32)
    return jnp.concatenate([a * cos - b * sin, b * cos + a * sin], -1).astype(jnp.bfloat16)


def matmul(a, w):
    return jnp.dot(a, w, preferred_element_type=jnp.float32).astype(jnp.bfloat16)


def einsum(form, a, b):
    return jnp.einsum(form, a.astype(jnp.float32), b.astype(jnp.float32))


def attention(q, k, v):
    scores = einsum("tgsd,ugd->gstu", q, k) * q.shape[-1] ** -0.5
    token = jnp.arange(q.shape[0])
    scores = jnp.where(token[:, None] >= token, scores, -jnp.inf)
    weights = jax.nn.softmax(scores, -1).astype(jnp.bfloat16)
    return einsum("gstu,ugd->tgsd", weights, v).astype(jnp.bfloat16)


def reference(x, gain, wq, wk, wv, wo):
    a, place = normed(x, gain), jnp.arange(ROWS)
    q = turned(matmul(a, wq).reshape(ROWS, HEADS, HEAD), place, THETA).reshape(ROWS, KV_HEADS, -1, HEAD)
    k = turned(matmul(a, wk).reshape(ROWS, KV_HEADS, HEAD), place, THETA)
    v = matmul(a, wv).reshape(ROWS, KV_HEADS, HEAD)
    seen = attention(q, k, v).reshape(ROWS, HEADS * HEAD)
    return (x.astype(jnp.float32) + jnp.dot(seen, wo, preferred_element_type=jnp.float32)).astype(jnp.bfloat16)
```

```python
import functools
import jax
import jax.numpy as jnp
import numpy as np
from jax import lax
from jax.experimental import pallas as pl
from jax.experimental.pallas import tpu as pltpu
from jax.sharding import PartitionSpec as P

VM=62*2**20
def rope(t, cs):
    c, s = cs[:, :64], cs[:, 64:]
    c2 = jnp.concatenate([c, c], 1); s2 = jnp.concatenate([-s, s], 1)
    return (t * c2 + pltpu.roll(t, 64, 1) * s2).astype(jnp.bfloat16)

def _qkv(x_ref, g_ref, cs_ref, wq_ref, wk_ref, wv_ref, q_ref, k_ref, v_ref, a_s):
    t = pl.program_id(0)
    last = pl.num_programs(0) - 1
    rows = x_ref.shape[0]
    @pl.when(t == 0)
    def _():
        for at in range(0, rows, 64):
            w = x_ref[at:at+64, :].astype(jnp.float32)
            sc = lax.rsqrt(jnp.mean(w*w, -1, keepdims=True) + 1e-6)
            a_s[at:at+64, :] = (w * sc * g_ref[...].astype(jnp.float32)).astype(jnp.bfloat16)
    a = a_s[...]
    cs = cs_ref[...]
    def emit(acc, out, turn, n):
        r = acc.astype(jnp.bfloat16)
        for i in range(n):
            p = r[:, i*128:(i+1)*128]
            out[i] = rope(p.astype(jnp.float32), cs) if turn else p
    @pl.when(t < last)
    def _():
        for w, o, turn in ((wq_ref, q_ref, True), (wk_ref, k_ref, True), (wv_ref, v_ref, False)):
            emit(jnp.dot(a, w[...], preferred_element_type=jnp.float32), o, turn, 2)
    @pl.when(t == last)
    def _():
        both = jnp.dot(a, jnp.concatenate([wq_ref[:, :128], wk_ref[:, :128]], 1), preferred_element_type=jnp.float32)
        emit(both[:, :128], q_ref, True, 1)
        emit(both[:, 128:], k_ref, True, 1)
        emit(jnp.dot(a, wv_ref[:, :128], preferred_element_type=jnp.float32), v_ref, False, 1)

def qkv(x, gain, cs, wq, wk, wv, at, rows):
    d = x.shape[1]; n = wq.shape[1]; heads = n // 128
    steps = -(-n // 256)
    b = at // rows
    wspec = pl.BlockSpec((d, 256), lambda t: (0, t))
    ospec = pl.BlockSpec((2, rows, 128), lambda t: (t, 0, 0))
    one = pl.Buffered(1)
    return pl.pallas_call(_qkv, grid=(steps,),
        in_specs=[pl.BlockSpec((rows, d), lambda t: (b, 0), pipeline_mode=one), pl.BlockSpec((1, d), lambda t: (0, 0)),
                  pl.BlockSpec((rows, 128), lambda t: (b, 0)), wspec, wspec, wspec],
        out_specs=[ospec]*3,
        out_shape=[jax.ShapeDtypeStruct((heads, rows, 128), jnp.bfloat16)]*3,
        scratch_shapes=[pltpu.VMEM((rows, d), jnp.bfloat16)],
        compiler_params=pltpu.CompilerParams(dimension_semantics=("arbitrary",), vmem_limit_bytes=VM),
        cost_estimate=pl.CostEstimate(flops=2*rows*d*3*n, bytes_accessed=2*(3*d*n+rows*d+3*rows*n), transcendentals=0),
        name="qkv",
    )(x, gain[None], cs, wq, wk, wv)

def _wo(half_ref, s0, s1, w0, w1, o):
    a = jnp.dot(s0[...], w0[...], preferred_element_type=jnp.float32)
    o[...] = (a + jnp.dot(s1[...], w1[...], preferred_element_type=jnp.float32)).astype(jnp.bfloat16)

def wo_mm(half, s0, s1, w0, w1, tile=256):
    rows, kk = s0.shape; n = w0.shape[1] // 2
    steps = n // tile
    wspec = pl.BlockSpec((kk, tile), lambda t, h: (0, h[0]*steps + t))
    sspec = pl.BlockSpec((rows, kk), lambda t, h: (0, 0))
    return pl.pallas_call(_wo, grid_spec=pltpu.PrefetchScalarGridSpec(num_scalar_prefetch=1, grid=(steps,),
        in_specs=[sspec, sspec, wspec, wspec], out_specs=pl.BlockSpec((rows, tile), lambda t, h: (0, t))),
        out_shape=jax.ShapeDtypeStruct((rows, n), jnp.bfloat16),
        compiler_params=pltpu.CompilerParams(dimension_semantics=("arbitrary",), vmem_limit_bytes=VM),
        cost_estimate=pl.CostEstimate(flops=2*rows*2*kk*n, bytes_accessed=2*(2*kk*n+2*rows*kk+rows*n), transcendentals=0),
        name="wo",
    )(half, s0, s1, w0, w1)

LOG2E=1.4426950408889634
HIDDEN=-1e30
def _dot(a, b, ca, cb):
    return lax.dot_general(a, b, (((ca,), (cb,)), ((), ())), preferred_element_type=jnp.float32)

def _attn(*refs, n, scale, hs):
    q_ref, ks, vs, o_ref = refs[0], refs[1:1+n], refs[1+n:1+2*n], refs[1+2*n]
    e = scale * LOG2E
    for h in range(hs):
        q = q_ref[h]
        ss = []
        for j in range(n):
            s = _dot(ks[j][h], q, 1, 1)
            if j == n-1:
                gap = lax.broadcasted_iota(jnp.int32, s.shape, 1) - lax.broadcasted_iota(jnp.int32, s.shape, 0)
                s = jnp.where(gap >= 0, s, HIDDEN)
            ss.append(s)
        top = functools.reduce(jnp.maximum, [s.max(axis=0, keepdims=True) for s in ss])
        acc = None
        for j in range(n):
            p = jnp.exp2((ss[j] - top) * e).astype(jnp.bfloat16)
            vt = jnp.concatenate([vs[j][h].T, jnp.ones((8, p.shape[0]), jnp.bfloat16)], 0)
            part = _dot(vt, p, 1, 0)
            acc = part if acc is None else acc + part
        out = acc[:128] * (1 / acc[128:129])
        o_ref[:, h*128:(h+1)*128] = out.T.astype(jnp.bfloat16)

def attn(q, ks, vs, hs=1):
    heads, rows, _ = q.shape
    n = len(ks)
    spec = lambda a: pl.BlockSpec((hs, a.shape[1], 128), lambda h: (h, 0, 0))
    keys = sum(k.shape[1] for k in ks)
    return pl.pallas_call(functools.partial(_attn, n=n, scale=128**-0.5, hs=hs), grid=(heads//hs,),
        in_specs=[spec(q)] + [spec(k) for k in ks] + [spec(v) for v in vs],
        out_specs=pl.BlockSpec((rows, hs*128), lambda h: (0, h)),
        out_shape=jax.ShapeDtypeStruct((rows, heads*128), jnp.bfloat16),
        compiler_params=pltpu.CompilerParams(dimension_semantics=("arbitrary",), vmem_limit_bytes=VM),
        cost_estimate=pl.CostEstimate(flops=4*heads*rows*keys*128, bytes_accessed=2*heads*128*(2*rows+2*keys), transcendentals=heads*rows*keys),
        name="attn",
    )(q, *ks, *vs)


def _finish(half_ref, x_ref, own, sib, rown, rsib, *ys):
    y_ref = ys[-1]
    n = own.shape[1]
    for c in range(2):
        @pl.when(half_ref[0] == c)
        def _():
            a, b = pl.ds(c * n, n), pl.ds((1 - c) * n, n)
            for cols, s, r in ((a, own, rown), (b, sib, rsib)):
                y_ref[:, cols] = (x_ref[:, cols].astype(jnp.float32) + (s[...].astype(jnp.float32) + r[...].astype(jnp.float32))).astype(jnp.bfloat16)

def finish(half, x, own, sib, rown, rsib, y, at):
    rows, n = own.shape; bm = 128
    wide = pl.BlockSpec((bm, 2*n), lambda t, h: (at//bm + t, 0))
    part = pl.BlockSpec((bm, n), lambda t, h: (t, 0))
    return pl.pallas_call(_finish, grid_spec=pltpu.PrefetchScalarGridSpec(num_scalar_prefetch=1, grid=(rows//bm,),
        in_specs=[wide, part, part, part, part] + [pl.BlockSpec(memory_space=pl.ANY)] * len(y), out_specs=wide),
        out_shape=jax.ShapeDtypeStruct(x.shape, jnp.bfloat16), input_output_aliases={6: 0} if y else {},
        compiler_params=pltpu.CompilerParams(dimension_semantics=("arbitrary",), vmem_limit_bytes=VM),
        cost_estimate=pl.CostEstimate(flops=rows*n*2000, bytes_accessed=rows*n*2*8, transcendentals=0),
        name="finish",
    )(half, x, own, sib, rown, rsib, *y)

def tables(rows):
    angle = np.arange(rows, dtype=np.float32)[:, None] * (10000.0 ** (-np.arange(64, dtype=np.float32) / 64)).astype(np.float32)
    return np.concatenate([np.cos(angle), np.sin(angle)], 1).astype(np.float32)

SIB = [(0, 1), (1, 0), (2, 3), (3, 2)]
CROSS = [(0, 2), (2, 0), (1, 3), (3, 1)]
CHUNKS = (512, 512, 512, 512)

def solution(mesh):
    def step(x, gain, wq, wk, wv, wo):
        rows = x.shape[0]
        cs = jnp.asarray(tables(rows))
        half = (lax.axis_index("tp") % 2).astype(jnp.int32)[None]
        wo_sib = lax.ppermute(wo, "tp", SIB)
        ks, vs, sums = [], [], []
        at = 0
        y = ()
        for r in CHUNKS:
            q, k, v = qkv(x, gain, cs, wq, wk, wv, at, r)
            ks.append(k); vs.append(v)
            seen = attn(q, ks, vs)
            seen_sib = lax.ppermute(seen, "tp", SIB)
            own = wo_mm(half, seen, seen_sib, wo, wo_sib)
            gain, own = lax.optimization_barrier((gain, own))
            rown = lax.ppermute(own, "tp", CROSS)
            sib = lax.ppermute(own, "tp", SIB)
            rsib = lax.ppermute(rown, "tp", SIB)
            sums.append((own, sib, rown, rsib, at))
            at += r
        for own, sib, rown, rsib, at in sums:
            y = (finish(half, x, own, sib, rown, rsib, y, at),)
        return y[0]

    tokens, columns = P("dp", None), P(None, "tp")
    return jax.shard_map(step, mesh=mesh, in_specs=(tokens, P(None), columns, columns, columns, P("tp", None)), out_specs=tokens, check_vma=False)
```

```python
import functools

import jax
import jax.numpy as jnp
import numpy as np
from jax import lax
from jax.experimental import pallas as pl
from jax.experimental.pallas import tpu as pltpu
from jax.sharding import PartitionSpec as P


HEAD = 128
VM = 62 * 2**20
LOG2E = 1.4426950408889634
HIDDEN = -1e30
HBM = pl.BlockSpec(memory_space=pltpu.HBM)
BF = jnp.bfloat16
SLOTS = 3


def _dot(a, b, ca, cb):
    return lax.dot_general(a, b, (((ca,), (cb,)), ((), ())), preferred_element_type=jnp.float32)


def _chunk(x_hbm, g_ref, cs_ref, wq, wk, wv, wo, *refs, at, n):
    old, refs = refs[: 2 * n], refs[2 * n :]
    w_sib, *refs = refs
    sum_out, k_out, v_out, x_s, a_s, w_s, p_s, seen_s, sa_s, sb_s, top_s = refs[:11]
    kv_s = refs[11 : 11 + 2 * n]
    x_sem, w_sem, kv_sem, out_sem, wo_sem, sum_sem, send_sem, recv_sem, ws_sem, wr_sem = refs[-10:]
    rows, _ = a_s.shape
    heads = (p_s.shape[0] - 1) // 3
    wide = w_s.shape[2]
    per = wide // HEAD
    full = 3 * (heads // per)
    slots = w_s.shape[0]
    piece = x_s.shape[1]
    n_pieces = rows // piece

    def load_x(i):
        return pltpu.make_async_copy(x_hbm.at[pl.ds(pl.multiple_of(at + i * piece, 64), piece), :], x_s.at[lax.rem(i, 2)], x_sem.at[lax.rem(i, 2)])

    def tile(m, p, slot):
        cols = pl.ds(pl.multiple_of(p * wide, wide), wide)
        return pltpu.make_async_copy((wq, wk, wv)[m].at[:, cols], w_s.at[slot], w_sem.at[slot])

    def lasts(slot):
        return [pltpu.make_async_copy(w.at[:, pl.ds((heads - 1) * HEAD, HEAD)], w_s.at[slot, :, pl.ds(i * HEAD, HEAD)], w_sem.at[slot]) for i, w in enumerate((wq, wk, wv))]

    def start(t):
        slot = lax.rem(t, slots)
        for m in range(3):
            @pl.when((t < full) & (lax.rem(t, 3) == m))
            def _():
                tile(m, t // 3, slot).start()

        @pl.when(t == full)
        def _():
            for c in lasts(slot):
                c.start()

    def wait(t):
        slot = lax.rem(t, slots)

        @pl.when(t < full)
        def _():
            tile(0, 0, slot).wait()

        @pl.when(t == full)
        def _():
            for c in lasts(slot):
                c.wait()

    me = lax.axis_index("tp")
    core = lax.rem(me, 2)
    sibling = {"tp": me + 1 - 2 * core}
    width = a_s.shape[1] // 2
    depth = heads * HEAD
    load_x(0).start()
    load_x(1).start()
    start(0)
    barrier = pltpu.get_barrier_semaphore()
    pl.semaphore_signal(barrier, inc=1, device_id=sibling, device_id_type=pl.DeviceIdType.MESH)
    pl.semaphore_wait(barrier, 1)
    give = None
    if n == 0:
        theirs = pl.ds(pl.multiple_of((1 - core) * width, HEAD), width)
        give = pltpu.make_async_remote_copy(wo.at[:, theirs], w_sib, ws_sem, wr_sem, device_id=sibling, device_id_type=pl.DeviceIdType.MESH)
    gain = g_ref[...].astype(jnp.float32)

    def norm(i, _):
        load_x(i).wait()
        for r in range(0, piece, 32):
            w = x_s[lax.rem(i, 2), r : r + 32, :].astype(jnp.float32)
            sc = lax.rsqrt(jnp.mean(w * w, -1, keepdims=True) + 1e-6)
            a_s[pl.ds(pl.multiple_of(i * piece + r, 32), 32), :] = (w * sc * gain).astype(BF)

        @pl.when(i + 2 < n_pieces)
        def _():
            load_x(i + 2).start()

        return 0

    lax.fori_loop(0, n_pieces, norm, 0)
    for t in range(1, slots - 1):
        start(t)
    if give is not None:
        give.start()
    kv = [pltpu.make_async_copy(src, dst, kv_sem.at[i]) for i, (src, dst) in enumerate(zip(old, kv_s))]

    def project_tile(t, _):
        wait(t)

        @pl.when(t + slots - 1 < full + 1)
        def _():
            start(t + slots - 1)

        acc = jnp.dot(a_s[...], w_s[lax.rem(t, slots)], preferred_element_type=jnp.float32)
        m = lax.rem(t, 3)
        cs = cs_ref[...]
        cos = jnp.concatenate([cs[:, :64], cs[:, :64]], 1)
        sin = jnp.concatenate([-cs[:, 64:], cs[:, 64:]], 1)
        for i in range(per):
            turn = jnp.where(t == full, i < 2, m < 2)
            to = m * heads + per * (t // 3) + i + (t // full) * ((heads - 1) * min(i, 2))
            v = acc[:, i * HEAD : (i + 1) * HEAD].astype(BF).astype(jnp.float32)
            p_s[to] = (v * jnp.where(turn, cos, 1.0) + pltpu.roll(v, 64, 1) * jnp.where(turn, sin, 0.0)).astype(BF)
        return 0

    lax.fori_loop(0, full - 1, project_tile, 0)
    for c in kv:
        c.start()
    lax.fori_loop(full - 1, full + 1, project_tile, 0)
    outs = [pltpu.make_async_copy(p_s.at[pl.ds(heads * (i + 1), heads)], o, out_sem.at[i]) for i, o in enumerate((k_out, v_out))]
    for c in outs:
        c.start()
    for c in kv:
        c.wait()

    e = HEAD**-0.5 * LOG2E
    parts = [(q0, min(256, rows - q0)) for q0 in range(0, rows, 256)]
    marks = [0]
    for j in range(n):
        marks.append(marks[-1] + kv_s[j].shape[1])
    own = marks[-1]

    def scores(h, s_s, row):
        for q0, ql in parts:
            q = p_s[h, q0 : q0 + ql, :]
            best = []
            for j in range(n):
                s = _dot(kv_s[j][h], q, 1, 1)
                s_s[marks[j] : marks[j + 1], q0 : q0 + ql] = s
                best.append(s.max(axis=0, keepdims=True))
            if q0:
                s = _dot(p_s[heads + h, :q0, :], q, 1, 1)
                s_s[own : own + q0, q0 : q0 + ql] = s
                best.append(s.max(axis=0, keepdims=True))
            s = _dot(p_s[heads + h, q0 : q0 + ql, :], q, 1, 1)
            gap = lax.broadcasted_iota(jnp.int32, s.shape, 1) - lax.broadcasted_iota(jnp.int32, s.shape, 0)
            s = jnp.where(gap >= 0, s, HIDDEN)
            s_s[own + q0 : own + q0 + ql, q0 : q0 + ql] = s
            best.append(s.max(axis=0, keepdims=True))
            top_s[row : row + 1, q0 : q0 + ql] = functools.reduce(jnp.maximum, best)

    def mix(h, s_s, row):
        def values(ref, i, size):
            return jnp.concatenate([ref[i, :size, :].T, jnp.ones((8, size), BF)], 0)

        vts = [values(kv_s[n + j], h, kv_s[n + j].shape[1]) for j in range(n)] + [values(p_s, 2 * heads + h, rows)]
        for q0, ql in parts:
            top = top_s[row : row + 1, q0 : q0 + ql]
            acc = None
            for j in range(n + 1):
                size = marks[j + 1] - marks[j] if j < n else q0 + ql
                p = jnp.exp2((s_s[marks[j] : marks[j] + size, q0 : q0 + ql] - top) * e).astype(BF)
                part = _dot(vts[j][:, :size], p, 1, 0)
                acc = part if acc is None else acc + part
            out = acc[:HEAD] * (1 / acc[HEAD : HEAD + 1])
            seen_s[q0 : q0 + ql, pl.ds(pl.multiple_of(h * HEAD, HEAD), HEAD)] = out.T.astype(BF)

    def send(i, size=2 * HEAD):
        at_ = pl.multiple_of(i * 2 * HEAD, HEAD)
        return pltpu.make_async_remote_copy(seen_s.at[:, pl.ds(at_, size)], seen_s.at[:, pl.ds(depth + at_, size)], send_sem.at[i], recv_sem.at[i],
                                            device_id=sibling, device_id_type=pl.DeviceIdType.MESH)

    tiles, rest = divmod(width, wide)

    def wo_tiles(t, cols=wide):
        slot = lax.rem(t, slots)
        mine = pl.ds(pl.multiple_of(core * width + t * wide, HEAD), cols)
        return [pltpu.make_async_copy(src, w_s.at[slot, pl.ds(i * depth, depth), pl.ds(0, cols)], wo_sem.at[slot, i])
                for i, src in enumerate((wo.at[:, mine], w_sib.at[:, pl.ds(pl.multiple_of(t * wide, HEAD), cols)]))]

    def put(t, cols=wide):
        span = pl.ds(pl.multiple_of(t * wide, HEAD), cols)
        return pltpu.make_async_copy(a_s.at[:, span], sum_out.at[:, span], sum_sem.at[t])

    scores(0, sa_s, 0)
    if give is not None:
        give.wait()
    for t in range(slots - 1):
        for c in wo_tiles(t):
            c.start()

    def two(i, _):
        scores(2 * i + 1, sb_s, 8)
        mix(2 * i, sa_s, 0)

        @pl.when(i > 0)
        def _():
            send(i - 1).start()

        scores(2 * i + 2, sa_s, 0)
        mix(2 * i + 1, sb_s, 8)
        return 0

    half_heads = heads // 2
    lax.fori_loop(0, half_heads, two, 0)
    send(half_heads - 1).start()
    mix(heads - 1, sa_s, 0)
    for c in wo_tiles(0):
        c.wait()
    send(half_heads, HEAD).start()
    lax.fori_loop(0, half_heads, lambda i, _: send(i).wait(), None)
    send(half_heads, HEAD).wait()

    def sum_tile(t, _):
        @pl.when(t > 0)
        def _():
            for c in wo_tiles(t):
                c.wait()
            put(t - 1).start()

        more = t + slots - 1

        @pl.when(more < tiles)
        def _():
            for c in wo_tiles(more):
                c.start()

        if rest:
            @pl.when(more == tiles)
            def _():
                for c in wo_tiles(tiles, rest):
                    c.start()

        acc = jnp.dot(seen_s[...], w_s[lax.rem(t, slots), : 2 * depth, :], preferred_element_type=jnp.float32)
        a_s[:, pl.ds(pl.multiple_of(t * wide, HEAD), wide)] = acc.astype(BF)
        return 0

    lax.fori_loop(0, tiles, sum_tile, 0)
    if rest:
        for c in wo_tiles(tiles, rest):
            c.wait()
        put(tiles - 1).start()
        a_s[:, tiles * wide : width] = jnp.dot(seen_s[...], w_s[tiles % slots, : 2 * depth, :rest], preferred_element_type=jnp.float32).astype(BF)
        put(tiles, rest).start()
        put(tiles, rest).wait()
    else:
        put(tiles - 1).start()
    for t in range(tiles):
        put(t).wait()
    for c in outs:
        c.wait()


def chunk(x, gain, cs, wq, wk, wv, wo, w_sib, ks, vs, at, rows):
    d, cols = wq.shape
    heads, n = cols // HEAD, len(ks)
    keys, half = at + rows, d // 2
    sib = jax.ShapeDtypeStruct((cols, half), BF)
    got = pl.pallas_call(
        functools.partial(_chunk, at=at, n=n),
        in_specs=[HBM, pl.BlockSpec((1, d), lambda: (0, 0)), pl.BlockSpec((rows, HEAD), lambda: (0, 0)), HBM, HBM, HBM, HBM] + [HBM] * (2 * n + (n > 0)),
        out_specs=[HBM] * (3 + (n == 0)),
        out_shape=[sib] * (n == 0) + [jax.ShapeDtypeStruct((rows, half), BF)] + [jax.ShapeDtypeStruct((heads, rows, HEAD), BF)] * 2,
        scratch_shapes=[pltpu.VMEM((2, 64, d), BF), pltpu.VMEM((rows, d), BF), pltpu.VMEM((SLOTS, d, 512), BF), pltpu.VMEM((3 * heads + 1, rows, HEAD), BF),
                        pltpu.VMEM((rows, 2 * cols), BF), pltpu.VMEM((keys, rows), jnp.float32), pltpu.VMEM((keys, rows), jnp.float32), pltpu.VMEM((16, rows), jnp.float32)]
        + [pltpu.VMEM(k.shape, BF) for k in (*ks, *vs)]
        + [pltpu.SemaphoreType.DMA((2,)), pltpu.SemaphoreType.DMA((SLOTS,)), pltpu.SemaphoreType.DMA((max(2 * n, 1),)), pltpu.SemaphoreType.DMA((2,)),
           pltpu.SemaphoreType.DMA((SLOTS, 2)), pltpu.SemaphoreType.DMA((half // 512 + 1,)), pltpu.SemaphoreType.DMA((heads // 2 + 1,)), pltpu.SemaphoreType.DMA((heads // 2 + 1,)),
           pltpu.SemaphoreType.DMA, pltpu.SemaphoreType.DMA],
        compiler_params=pltpu.CompilerParams(vmem_limit_bytes=VM, collective_id=n, has_side_effects=True),
        cost_estimate=pl.CostEstimate(flops=2 * rows * d * (3 * cols + 2 * cols) + 4 * rows * keys * cols, transcendentals=heads * rows * keys,
                                      bytes_accessed=2 * (5 * d * cols + rows * d + 3 * rows * cols + 2 * keys * cols)),
        name="chunk",
    )(x, gain[None], cs[at : at + rows], wq, wk, wv, wo, *ks, *vs, *([] if n == 0 else [w_sib]))
    return got if n == 0 else (w_sib, *got)


def _finish(half_ref, x_ref, own, sib, rown, rsib, *ys):
    y_ref = ys[-1]
    n = own.shape[1]
    for c in range(2):
        @pl.when(half_ref[0] == c)
        def _():
            a, b = pl.ds(c * n, n), pl.ds((1 - c) * n, n)
            for cols, s, r in ((a, own, rown), (b, sib, rsib)):
                y_ref[:, cols] = (x_ref[:, cols].astype(jnp.float32) + (s[...].astype(jnp.float32) + r[...].astype(jnp.float32))).astype(BF)


def finish(half, x, own, sib, rown, rsib, y, at):
    rows, n = own.shape
    bm = 64
    wide = pl.BlockSpec((bm, 2 * n), lambda t, h: (at // bm + t, 0))
    part = pl.BlockSpec((bm, n), lambda t, h: (t, 0))
    return pl.pallas_call(
        _finish,
        grid_spec=pltpu.PrefetchScalarGridSpec(num_scalar_prefetch=1, grid=(rows // bm,), in_specs=[wide, part, part, part, part] + [HBM] * len(y), out_specs=wide),
        out_shape=jax.ShapeDtypeStruct(x.shape, BF),
        input_output_aliases={6: 0} if y else {},
        compiler_params=pltpu.CompilerParams(dimension_semantics=("arbitrary",)),
        cost_estimate=pl.CostEstimate(flops=rows * n * 2000, bytes_accessed=rows * n * 2 * 8, transcendentals=0),
        name="finish",
    )(half, x, own, sib, rown, rsib, *y)


def tables(rows):
    angle = np.arange(rows, dtype=np.float32)[:, None] * (10000.0 ** (-np.arange(64, dtype=np.float32) / 64)).astype(np.float32)
    return np.concatenate([np.cos(angle), np.sin(angle)], 1).astype(np.float32)


SIB = [(0, 1), (1, 0), (2, 3), (3, 2)]
CROSS = [(0, 2), (2, 0), (1, 3), (3, 1)]
CHUNKS = (384, 512, 512, 384, 256)


def solution(mesh):
    def step(x, gain, wq, wk, wv, wo):
        cs = jnp.asarray(tables(x.shape[0]))
        half = (lax.axis_index("tp") % 2).astype(jnp.int32)[None]
        ks, vs, sums = [], [], []
        w_sib, at = None, 0
        for rows in CHUNKS:
            w_sib, own, k, v = chunk(x, gain, cs, wq, wk, wv, wo, w_sib, ks, vs, at, rows)
            ks.append(k)
            vs.append(v)
            gain, own = lax.optimization_barrier((gain, own))
            rown = lax.ppermute(own, "tp", CROSS)
            sib = lax.ppermute(own, "tp", SIB)
            rsib = lax.ppermute(rown, "tp", SIB)
            sums.append((own, sib, rown, rsib, at))
            at += rows
        y = ()
        for own, sib, rown, rsib, at in sums:
            y = (finish(half, x, own, sib, rown, rsib, y, at),)
        return y[0]

    tokens, columns = P("dp", None), P(None, "tp")
    return jax.shard_map(step, mesh=mesh, in_specs=(tokens, P(None), columns, columns, columns, P("tp", None)), out_specs=tokens, check_vma=False)
```

```python
import functools

import jax
import jax.numpy as jnp
import numpy as np
from jax import lax
from jax.experimental import pallas as pl
from jax.experimental.pallas import tpu as pltpu
from jax.sharding import PartitionSpec as P


HEAD = 128
VM = 62 * 2**20
LOG2E = 1.4426950408889634
HIDDEN = -1e30
HBM = pl.BlockSpec(memory_space=pltpu.HBM)
BF = jnp.bfloat16
SLOTS = 3


def _dot(a, b, ca, cb):
    return lax.dot_general(a, b, (((ca,), (cb,)), ((), ())), preferred_element_type=jnp.float32)


def _chunk(x_hbm, g_ref, cs_ref, wq, wk, wv, wo, *refs, at, n, n_sums):
    old, refs = refs[: 2 * n], refs[2 * n :]
    w_sib, *refs = refs
    sums, refs = refs[:n_sums], refs[n_sums:]
    k_out, v_out, x_s, a_s, w_s, p_s, seen_s, sa_s, sb_s, top_s, raw_s = refs[:11]
    kv_s = refs[11 : 11 + 2 * n]
    x_sem, w_sem, kv_sem, out_sem, wo_sem, sum_sem, send_sem, recv_sem, ws_sem, wr_sem = refs[-10:]
    rows, _ = a_s.shape
    heads = (p_s.shape[0] - 1) // 3
    wide = w_s.shape[2]
    per = wide // HEAD
    full = 3 * (heads // per)
    slots = w_s.shape[0]
    piece = x_s.shape[1]
    n_pieces = rows // piece

    def load_x(i):
        return pltpu.make_async_copy(x_hbm.at[pl.ds(pl.multiple_of(at + i * piece, 64), piece), :], x_s.at[lax.rem(i, 2)], x_sem.at[lax.rem(i, 2)])

    def tile(m, p, slot):
        cols = pl.ds(pl.multiple_of(p * wide, wide), wide)
        return pltpu.make_async_copy((wq, wk, wv)[m].at[:, cols], w_s.at[slot], w_sem.at[slot])

    def lasts(slot):
        return [pltpu.make_async_copy(w.at[:, pl.ds((heads - 1) * HEAD, HEAD)], w_s.at[slot, :, pl.ds(i * HEAD, HEAD)], w_sem.at[slot]) for i, w in enumerate((wq, wk, wv))]

    def start(t):
        slot = lax.rem(t, slots)
        for m in range(3):
            @pl.when((t < full) & (lax.rem(t, 3) == m))
            def _():
                tile(m, t // 3, slot).start()

        @pl.when(t == full)
        def _():
            for c in lasts(slot):
                c.start()

    def wait(t):
        slot = lax.rem(t, slots)

        @pl.when(t < full)
        def _():
            tile(0, 0, slot).wait()

        @pl.when(t == full)
        def _():
            for c in lasts(slot):
                c.wait()

    me = lax.axis_index("tp")
    core = lax.rem(me, 2)
    sibling = {"tp": me + 1 - 2 * core}
    width = a_s.shape[1] // 2
    depth = heads * HEAD
    load_x(0).start()
    load_x(1).start()
    start(0)
    barrier = pltpu.get_barrier_semaphore()
    pl.semaphore_signal(barrier, inc=1, device_id=sibling, device_id_type=pl.DeviceIdType.MESH)
    pl.semaphore_wait(barrier, 1)
    give = None
    if n == 0:
        theirs = pl.ds(pl.multiple_of((1 - core) * width, HEAD), width)
        give = pltpu.make_async_remote_copy(wo.at[:, theirs], w_sib, ws_sem, wr_sem, device_id=sibling, device_id_type=pl.DeviceIdType.MESH)
    gain = g_ref[...].astype(jnp.float32)

    def norm(i, _):
        load_x(i).wait()

        def few(r, _):
            w = x_s[lax.rem(i, 2), pl.ds(pl.multiple_of(r * 32, 32), 32), :].astype(jnp.float32)
            sc = lax.rsqrt(jnp.mean(w * w, -1, keepdims=True) + 1e-6)
            a_s[pl.ds(pl.multiple_of(i * piece + r * 32, 32), 32), :] = (w * sc * gain).astype(BF)
            return 0

        lax.fori_loop(0, piece // 32, few, 0)

        @pl.when(i + 2 < n_pieces)
        def _():
            load_x(i + 2).start()

        return 0

    lax.fori_loop(0, n_pieces, norm, 0)
    for t in range(1, slots - 1):
        start(t)
    if give is not None:
        give.start()
    kv = [pltpu.make_async_copy(src, dst, kv_sem.at[i]) for i, (src, dst) in enumerate(zip(old, kv_s))]

    def project_tile(t, _):
        wait(t)

        @pl.when(t + slots - 1 < full + 1)
        def _():
            start(t + slots - 1)

        if n:
            @pl.when(t == full - 1)
            def _():
                for c in kv:
                    c.start()

        turn_tile(t - (t + full) // (full + 1))
        raw_s[...] = jnp.dot(a_s[...], w_s[lax.rem(t, slots)], preferred_element_type=jnp.float32).astype(BF)
        return 0

    def turn_tile(t):
        m = lax.rem(t, 3)
        cs = cs_ref[...]
        cos = jnp.concatenate([cs[:, :64], cs[:, :64]], 1)
        sin = jnp.concatenate([-cs[:, 64:], cs[:, 64:]], 1)
        for i in range(per):
            turn = jnp.where(t == full, i < 2, m < 2)
            to = m * heads + per * (t // 3) + i + (t // full) * ((heads - 1) * min(i, 2))
            v = raw_s[:, i * HEAD : (i + 1) * HEAD].astype(jnp.float32)
            p_s[to] = (v * jnp.where(turn, cos, 1.0) + pltpu.roll(v, 64, 1) * jnp.where(turn, sin, 0.0)).astype(BF)

    lax.fori_loop(0, full + 1, project_tile, 0)
    turn_tile(full)
    outs = [pltpu.make_async_copy(p_s.at[pl.ds(heads * (i + 1), heads)], o, out_sem.at[i]) for i, o in enumerate((k_out, v_out))]
    for c in outs:
        c.start()
    for c in kv:
        c.wait()

    e = HEAD**-0.5 * LOG2E
    parts = [(q0, min(256, rows - q0)) for q0 in range(0, rows, 256)]
    marks = [0]
    for j in range(n):
        marks.append(marks[-1] + kv_s[j].shape[1])
    own = marks[-1]

    def scores(h, s_s, row):
        for q0, ql in parts:
            q = p_s[h, q0 : q0 + ql, :]
            best = []
            for j in range(n):
                s = _dot(kv_s[j][h], q, 1, 1)
                s_s[marks[j] : marks[j + 1], q0 : q0 + ql] = s
                best.append(s.max(axis=0, keepdims=True))
            if q0:
                s = _dot(p_s[heads + h, :q0, :], q, 1, 1)
                s_s[own : own + q0, q0 : q0 + ql] = s
                best.append(s.max(axis=0, keepdims=True))
            s = _dot(p_s[heads + h, q0 : q0 + ql, :], q, 1, 1)
            gap = lax.broadcasted_iota(jnp.int32, s.shape, 1) - lax.broadcasted_iota(jnp.int32, s.shape, 0)
            s = jnp.where(gap >= 0, s, HIDDEN)
            s_s[own + q0 : own + q0 + ql, q0 : q0 + ql] = s
            best.append(s.max(axis=0, keepdims=True))
            top_s[row : row + 1, q0 : q0 + ql] = functools.reduce(jnp.maximum, best)

    def mix(h, s_s, row):
        def values(ref, i, size):
            return jnp.concatenate([ref[i, :size, :].T, jnp.ones((8, size), BF)], 0)

        vts = [values(kv_s[n + j], h, kv_s[n + j].shape[1]) for j in range(n)] + [values(p_s, 2 * heads + h, rows)]
        for q0, ql in parts:
            top = top_s[row : row + 1, q0 : q0 + ql]
            acc = None
            for j in range(n + 1):
                size = marks[j + 1] - marks[j] if j < n else q0 + ql
                p = jnp.exp2((s_s[marks[j] : marks[j] + size, q0 : q0 + ql] - top) * e).astype(BF)
                part = _dot(vts[j][:, :size], p, 1, 0)
                acc = part if acc is None else acc + part
            out = acc[:HEAD] * (1 / acc[HEAD : HEAD + 1])
            seen_s[q0 : q0 + ql, pl.ds(pl.multiple_of(h * HEAD, HEAD), HEAD)] = out.T.astype(BF)

    def send(i, size=2 * HEAD):
        at_ = pl.multiple_of(i * 2 * HEAD, HEAD)
        return pltpu.make_async_remote_copy(seen_s.at[:, pl.ds(at_, size)], seen_s.at[:, pl.ds(depth + at_, size)], send_sem.at[i], recv_sem.at[i],
                                            device_id=sibling, device_id_type=pl.DeviceIdType.MESH)

    tiles = -(-width // wide)
    over = tiles * wide - width

    def wo_tiles(t):
        slot = lax.rem(t, slots)
        col = t * wide - (t // (tiles - 1)) * over
        return [pltpu.make_async_copy(src, w_s.at[slot, pl.ds(i * depth, depth), :], wo_sem.at[slot, i])
                for i, src in enumerate((wo.at[:, pl.ds(pl.multiple_of(core * width + col, HEAD), wide)], w_sib.at[:, pl.ds(pl.multiple_of(col, HEAD), wide)]))]

    def put(t, cols=wide):
        span = pl.ds(pl.multiple_of(t * wide, HEAD), cols)
        size = rows // n_sums
        return [pltpu.make_async_copy(a_s.at[pl.ds(i * size, size), span], out.at[:, span], sum_sem.at[t, i]) for i, out in enumerate(sums)]

    scores(0, sa_s, 0)
    scores(1, sb_s, 8)
    if give is not None:
        give.wait()
    for t in range(slots - 1):
        for c in wo_tiles(t):
            c.start()

    def two(i, _):
        mix(2 * i, sa_s, 0)
        mix(2 * i + 1, sb_s, 8)
        scores(2 * i + 2, sa_s, 0)
        scores(2 * i + 3 - (2 * i + 3) // heads, sb_s, 8)

        @pl.when(i > 0)
        def _():
            send(i - 1).start()

        return 0

    half_heads = heads // 2
    lax.fori_loop(0, half_heads, two, 0)
    send(half_heads - 1).start()
    mix(heads - 1, sa_s, 0)
    for c in wo_tiles(0):
        c.wait()
    send(half_heads, HEAD).start()
    lax.fori_loop(0, half_heads, lambda i, _: send(i).wait(), None)
    send(half_heads, HEAD).wait()

    def sum_tile(t, _):
        @pl.when(t > 0)
        def _():
            for c in wo_tiles(t):
                c.wait()
            for c in put(t - 1):
                c.start()

        more = t + slots - 1

        @pl.when(more < tiles)
        def _():
            for c in wo_tiles(more):
                c.start()

        acc = jnp.dot(seen_s[...], w_s[lax.rem(t, slots), : 2 * depth, :], preferred_element_type=jnp.float32)
        acc = acc.astype(BF)

        @pl.when(t < tiles - 1)
        def _():
            a_s[:, pl.ds(pl.multiple_of(t * wide, HEAD), wide)] = acc

        @pl.when(t == tiles - 1)
        def _():
            a_s[:, (tiles - 1) * wide : width] = acc[:, over:]

        return 0

    lax.fori_loop(0, tiles, sum_tile, 0)
    for c in put(tiles - 1, wide - over):
        c.start()
    for t in range(tiles - 1):
        for c in put(t):
            c.wait()
    for c in put(tiles - 1, wide - over):
        c.wait()
    for c in outs:
        c.wait()


def chunk(x, gain, cs, wq, wk, wv, wo, w_sib, ks, vs, at, rows, split):
    d, cols = wq.shape
    heads, n = cols // HEAD, len(ks)
    keys, half = at + rows, d // 2
    sib = jax.ShapeDtypeStruct((cols, half), BF)
    got = pl.pallas_call(
        functools.partial(_chunk, at=at, n=n, n_sums=split),
        in_specs=[HBM, pl.BlockSpec((1, d), lambda: (0, 0)), pl.BlockSpec((rows, HEAD), lambda: (0, 0)), HBM, HBM, HBM, HBM] + [HBM] * (2 * n + (n > 0)),
        out_specs=[HBM] * (2 + split + (n == 0)),
        out_shape=[sib] * (n == 0) + [jax.ShapeDtypeStruct((rows // split, half), BF)] * split + [jax.ShapeDtypeStruct((heads, rows, HEAD), BF)] * 2,
        scratch_shapes=[pltpu.VMEM((2, 64, d), BF), pltpu.VMEM((rows, d), BF), pltpu.VMEM((SLOTS, d, 512), BF), pltpu.VMEM((3 * heads + 1, rows, HEAD), BF),
                        pltpu.VMEM((rows, 2 * cols), BF), pltpu.VMEM((keys, rows), jnp.float32), pltpu.VMEM((keys, rows), jnp.float32), pltpu.VMEM((16, rows), jnp.float32), pltpu.VMEM((rows, 512), BF)]
        + [pltpu.VMEM(k.shape, BF) for k in (*ks, *vs)]
        + [pltpu.SemaphoreType.DMA((2,)), pltpu.SemaphoreType.DMA((SLOTS,)), pltpu.SemaphoreType.DMA((max(2 * n, 1),)), pltpu.SemaphoreType.DMA((2,)),
           pltpu.SemaphoreType.DMA((SLOTS, 2)), pltpu.SemaphoreType.DMA((half // 512 + 1, split)), pltpu.SemaphoreType.DMA((heads // 2 + 1,)), pltpu.SemaphoreType.DMA((heads // 2 + 1,)),
           pltpu.SemaphoreType.DMA, pltpu.SemaphoreType.DMA],
        compiler_params=pltpu.CompilerParams(vmem_limit_bytes=VM, collective_id=n, has_side_effects=True),
        cost_estimate=pl.CostEstimate(flops=2 * rows * d * (3 * cols + 2 * cols) + 4 * rows * keys * cols, transcendentals=heads * rows * keys,
                                      bytes_accessed=2 * (5 * d * cols + rows * d + 3 * rows * cols + 2 * keys * cols)),
        name="chunk",
    )(x, gain, cs[at : at + rows], wq, wk, wv, wo, *ks, *vs, *([] if n == 0 else [w_sib]))
    got = got if n == 0 else (w_sib, *got)
    return got[0], got[1:-2], got[-2], got[-1]


def _finish(half_ref, x_ref, own, sib, rown, rsib, *ys):
    y_ref = ys[-1]
    n = own.shape[1]
    for c in range(2):
        @pl.when(half_ref[0] == c)
        def _():
            def few(i, _):
                r = pl.ds(pl.multiple_of(i * 16, 16), 16)
                for cols, s, o in ((pl.ds(c * n, n), own, rown), (pl.ds((1 - c) * n, n), sib, rsib)):
                    y_ref[r, cols] = (x_ref[r, cols].astype(jnp.float32) + (s[r, :].astype(jnp.float32) + o[r, :].astype(jnp.float32))).astype(BF)
                return 0

            lax.fori_loop(0, y_ref.shape[0] // 16, few, 0)


def finish(half, x, own, sib, rown, rsib, y, at):
    rows, n = own.shape
    bm = 64
    wide = pl.BlockSpec((bm, 2 * n), lambda t, h: (at // bm + t, 0))
    part = pl.BlockSpec((bm, n), lambda t, h: (t, 0))
    return pl.pallas_call(
        _finish,
        grid_spec=pltpu.PrefetchScalarGridSpec(num_scalar_prefetch=1, grid=(rows // bm,), in_specs=[wide, part, part, part, part] + [HBM] * len(y), out_specs=wide),
        out_shape=jax.ShapeDtypeStruct(x.shape, BF),
        input_output_aliases={6: 0} if y else {},
        compiler_params=pltpu.CompilerParams(dimension_semantics=("arbitrary",)),
        cost_estimate=pl.CostEstimate(flops=rows * n * 2000, bytes_accessed=rows * n * 2 * 8, transcendentals=0),
        name="finish",
    )(half, x, own, sib, rown, rsib, *y)


def tables(rows):
    angle = np.arange(rows, dtype=np.float32)[:, None] * (10000.0 ** (-np.arange(64, dtype=np.float32) / 64)).astype(np.float32)
    return np.concatenate([np.cos(angle), np.sin(angle)], 1).astype(np.float32)


SIB = [(0, 1), (1, 0), (2, 3), (3, 2)]
CROSS = [(0, 2), (2, 0), (1, 3), (3, 1)]
CHUNKS = ((384, 1), (512, 1), (512, 1), (384, 1), (256, 2))


def solution(mesh):
    def step(x, gain, wq, wk, wv, wo):
        cs = jnp.asarray(tables(x.shape[0]))
        half = (lax.axis_index("tp") % 2).astype(jnp.int32)[None]
        gain = gain[None]
        ks, vs, sums = [], [], []
        w_sib, at = None, 0
        for rows, split in CHUNKS:
            w_sib, owns, k, v = chunk(x, gain, cs, wq, wk, wv, wo, w_sib, ks, vs, at, rows, split)
            ks.append(k)
            vs.append(v)
            gain, owns = lax.optimization_barrier((gain, owns))
            for own in owns:
                rown = lax.ppermute(own, "tp", CROSS)
                sib = lax.ppermute(own, "tp", SIB)
                rsib = lax.ppermute(rown, "tp", SIB)
                sums.append((own, sib, rown, rsib, at))
                at += rows // split
        y = ()
        for own, sib, rown, rsib, at in sums:
            y = (finish(half, x, own, sib, rown, rsib, y, at),)
        return y[0]

    tokens, columns = P("dp", None), P(None, "tp")
    return jax.shard_map(step, mesh=mesh, in_specs=(tokens, P(None), columns, columns, columns, P("tp", None)), out_specs=tokens, check_vma=False)
```

```python
import functools

import jax
import jax.numpy as jnp
import numpy as np
from jax import lax
from jax.experimental import pallas as pl
from jax.experimental.pallas import tpu as pltpu
from jax.sharding import PartitionSpec as P


HEAD = 128
VM = 62 * 2**20
LOG2E = 1.4426950408889634
HIDDEN = -1e30
HBM = pl.BlockSpec(memory_space=pltpu.HBM)
BF = jnp.bfloat16
SLOTS = 3


def _dot(a, b, ca, cb):
    return lax.dot_general(a, b, (((ca,), (cb,)), ((), ())), preferred_element_type=jnp.float32)


def _chunk(x_hbm, g_ref, cs_ref, wq, wk, wv, wo, *refs, at, n, n_sums):
    old, refs = refs[: 2 * n], refs[2 * n :]
    w_sib, *refs = refs
    sums, refs = refs[:n_sums], refs[n_sums:]
    k_out, v_out, x_s, a_s, w_s, p_s, seen_s, sa_s, sb_s, top_s, raw_s = refs[:11]
    kv_s = refs[11 : 11 + 2 * n]
    x_sem, w_sem, kv_sem, out_sem, wo_sem, sum_sem, send_sem, recv_sem, ws_sem, wr_sem = refs[-10:]
    rows, _ = a_s.shape
    heads = (p_s.shape[0] - 1) // 3
    wide = w_s.shape[2]
    per = wide // HEAD
    full = 3 * (heads // per)
    slots = w_s.shape[0]
    piece = x_s.shape[1]
    n_pieces = rows // piece

    def load_x(i):
        return pltpu.make_async_copy(x_hbm.at[pl.ds(pl.multiple_of(at + i * piece, 64), piece), :], x_s.at[lax.rem(i, 4)], x_sem.at[lax.rem(i, 4)])

    def tile(m, p, slot):
        cols = pl.ds(pl.multiple_of(p * wide, wide), wide)
        return pltpu.make_async_copy((wq, wk, wv)[m].at[:, cols], w_s.at[slot], w_sem.at[slot])

    def lasts(slot):
        return [pltpu.make_async_copy(w.at[:, pl.ds((heads - 1) * HEAD, HEAD)], w_s.at[slot, :, pl.ds(i * HEAD, HEAD)], w_sem.at[slot]) for i, w in enumerate((wq, wk, wv))]

    def start(t):
        slot = lax.rem(t, slots)
        for m in range(3):
            @pl.when((t < full) & (lax.rem(t, 3) == m))
            def _():
                tile(m, t // 3, slot).start()

        @pl.when(t == full)
        def _():
            for c in lasts(slot):
                c.start()

    def wait(t):
        slot = lax.rem(t, slots)

        @pl.when(t < full)
        def _():
            tile(0, 0, slot).wait()

        @pl.when(t == full)
        def _():
            for c in lasts(slot):
                c.wait()

    me = lax.axis_index("tp")
    core = lax.rem(me, 2)
    sibling = {"tp": me + 1 - 2 * core}
    width = a_s.shape[1] // 2
    depth = heads * HEAD
    for i in range(min(4, n_pieces)):
        load_x(i).start()
    start(0)
    barrier = pltpu.get_barrier_semaphore()
    pl.semaphore_signal(barrier, inc=1, device_id=sibling, device_id_type=pl.DeviceIdType.MESH)
    pl.semaphore_wait(barrier, 1)
    shares = -(-width // wide)

    def give(j, cols=wide):
        col = pl.multiple_of(j * wide, HEAD)
        return pltpu.make_async_remote_copy(wo.at[:, pl.ds(pl.multiple_of((1 - core) * width + col, HEAD), cols)], w_sib.at[:, pl.ds(col, cols)],
                                            ws_sem.at[j], wr_sem.at[j], device_id=sibling, device_id_type=pl.DeviceIdType.MESH)

    gives = [(j, min(wide, width - j * wide)) for j in range(shares)]
    gain = g_ref[...].astype(jnp.float32)[None]

    def norm(i, _):
        load_x(i).wait()

        def few(r, _):
            w = x_s[lax.rem(i, 4), pl.ds(pl.multiple_of(r * 32, 32), 32), :].astype(jnp.float32)
            sc = lax.rsqrt(jnp.mean(w * w, -1, keepdims=True) + 1e-6)
            a_s[pl.ds(pl.multiple_of(i * piece + r * 32, 32), 32), :] = (w * sc * gain).astype(BF)
            return 0

        lax.fori_loop(0, piece // 32, few, 0)

        @pl.when(i + 4 < n_pieces)
        def _():
            load_x(i + 4).start()

        return 0

    lax.fori_loop(0, n_pieces, norm, 0)
    for t in range(1, slots - 1):
        start(t)
    if n == 0:
        for j, cols in gives[:2]:
            give(j, cols).start()
    kv = [pltpu.make_async_copy(src, dst, kv_sem.at[i]) for i, (src, dst) in enumerate(zip(old, kv_s))]

    def project_tile(t, _):
        wait(t)

        @pl.when(t + slots - 1 < full + 1)
        def _():
            start(t + slots - 1)

        if n == 0:
            for j, cols in gives[2:]:
                @pl.when(t == j)
                def _():
                    give(j, cols).start()

        if n:
            @pl.when(t == full - 1)
            def _():
                for c in kv:
                    c.start()

        turn_tile(t - (t + full) // (full + 1))
        raw_s[...] = jnp.dot(a_s[...], w_s[lax.rem(t, slots)], preferred_element_type=jnp.float32).astype(BF)
        return 0

    def turn_tile(t):
        m = lax.rem(t, 3)
        cs = cs_ref[...]
        cos = jnp.concatenate([cs[:, :64], cs[:, :64]], 1)
        sin = jnp.concatenate([-cs[:, 64:], cs[:, 64:]], 1)
        for i in range(per):
            turn = jnp.where(t == full, i < 2, m < 2)
            to = m * heads + per * (t // 3) + i + (t // full) * ((heads - 1) * min(i, 2))
            v = raw_s[:, i * HEAD : (i + 1) * HEAD].astype(jnp.float32)
            p_s[to] = (v * jnp.where(turn, cos, 1.0) + pltpu.roll(v, 64, 1) * jnp.where(turn, sin, 0.0)).astype(BF)

    lax.fori_loop(0, full + 1, project_tile, 0)
    turn_tile(full)
    outs = [pltpu.make_async_copy(p_s.at[pl.ds(heads * (i + 1), heads)], o, out_sem.at[i]) for i, o in enumerate((k_out, v_out))]
    for c in outs:
        c.start()
    for c in kv:
        c.wait()

    e = HEAD**-0.5 * LOG2E
    parts = [(q0, min(256, rows - q0)) for q0 in range(0, rows, 256)]
    marks = [0]
    for j in range(n):
        marks.append(marks[-1] + kv_s[j].shape[1])
    own = marks[-1]

    def scores(h, s_s, row):
        for q0, ql in parts:
            q = p_s[h, q0 : q0 + ql, :]
            best = []
            for j in range(n):
                s = _dot(kv_s[j][h], q, 1, 1)
                s_s[marks[j] : marks[j + 1], q0 : q0 + ql] = s
                best.append(s.max(axis=0, keepdims=True))
            if q0:
                s = _dot(p_s[heads + h, :q0, :], q, 1, 1)
                s_s[own : own + q0, q0 : q0 + ql] = s
                best.append(s.max(axis=0, keepdims=True))
            s = _dot(p_s[heads + h, q0 : q0 + ql, :], q, 1, 1)
            gap = lax.broadcasted_iota(jnp.int32, s.shape, 1) - lax.broadcasted_iota(jnp.int32, s.shape, 0)
            s = jnp.where(gap >= 0, s, HIDDEN)
            s_s[own + q0 : own + q0 + ql, q0 : q0 + ql] = s
            best.append(s.max(axis=0, keepdims=True))
            top_s[row : row + 1, q0 : q0 + ql] = functools.reduce(jnp.maximum, best)

    def mix(h, s_s, row):
        def values(ref, i, size):
            return jnp.concatenate([ref[i, :size, :].T, jnp.ones((8, size), BF)], 0)

        vts = [values(kv_s[n + j], h, kv_s[n + j].shape[1]) for j in range(n)] + [values(p_s, 2 * heads + h, rows)]
        for q0, ql in parts:
            top = top_s[row : row + 1, q0 : q0 + ql]
            acc = None
            for j in range(n + 1):
                size = marks[j + 1] - marks[j] if j < n else q0 + ql
                p = jnp.exp2((s_s[marks[j] : marks[j] + size, q0 : q0 + ql] - top) * e).astype(BF)
                part = _dot(vts[j][:, :size], p, 1, 0)
                acc = part if acc is None else acc + part
            out = acc[:HEAD] * (1 / acc[HEAD : HEAD + 1])
            seen_s[q0 : q0 + ql, pl.ds(pl.multiple_of(h * HEAD, HEAD), HEAD)] = out.T.astype(BF)

    def send(i, size=2 * HEAD):
        at_ = pl.multiple_of(i * 2 * HEAD, HEAD)
        return pltpu.make_async_remote_copy(seen_s.at[:, pl.ds(at_, size)], seen_s.at[:, pl.ds(depth + at_, size)], send_sem.at[i], recv_sem.at[i],
                                            device_id=sibling, device_id_type=pl.DeviceIdType.MESH)

    tiles = -(-width // wide)
    over = tiles * wide - width

    wo_slots = 2 * slots

    def wo_tiles(t):
        slot = lax.rem(t, wo_slots)
        col = t * wide - (t // (tiles - 1)) * over
        return [pltpu.make_async_copy(src, w_s.at[slot // 2, pl.ds(lax.rem(slot, 2) * (2 * depth) + i * depth, depth), :], wo_sem.at[slot, i])
                for i, src in enumerate((wo.at[:, pl.ds(pl.multiple_of(core * width + col, HEAD), wide)], w_sib.at[:, pl.ds(pl.multiple_of(col, HEAD), wide)]))]

    def put(t, cols=wide):
        span = pl.ds(pl.multiple_of(t * wide, HEAD), cols)
        size = rows // n_sums
        return [pltpu.make_async_copy(a_s.at[pl.ds(i * size, size), span], out.at[:, span], sum_sem.at[t, i]) for i, out in enumerate(sums)]

    scores(0, sa_s, 0)
    scores(1, sb_s, 8)
    for t in range(min(tiles, wo_slots)):
        if n == 0:
            give(*gives[t]).wait()
        for c in wo_tiles(t):
            c.start()
    if n == 0:
        for j, cols in gives[wo_slots:]:
            give(j, cols).wait()

    def two(i, _):
        mix(2 * i, sa_s, 0)
        mix(2 * i + 1, sb_s, 8)
        scores(2 * i + 2, sa_s, 0)
        scores(2 * i + 3 - (2 * i + 3) // heads, sb_s, 8)

        @pl.when(i > 0)
        def _():
            send(i - 1).start()

        return 0

    half_heads = heads // 2
    lax.fori_loop(0, half_heads, two, 0)
    send(half_heads - 1).start()
    mix(heads - 1, sa_s, 0)
    for c in wo_tiles(0):
        c.wait()
    send(half_heads, HEAD).start()
    lax.fori_loop(0, half_heads, lambda i, _: send(i).wait(), None)
    send(half_heads, HEAD).wait()

    def sum_tile(t, _):
        @pl.when(t > 0)
        def _():
            for c in wo_tiles(t):
                c.wait()
            for c in put(t - 1):
                c.start()

        slot = lax.rem(t, wo_slots)
        w = w_s[slot // 2, pl.ds(pl.multiple_of(lax.rem(slot, 2) * (2 * depth), 16), 2 * depth), :]
        acc = jnp.dot(seen_s[...], w, preferred_element_type=jnp.float32).astype(BF)

        @pl.when(t + wo_slots < tiles)
        def _():
            for c in wo_tiles(t + wo_slots):
                c.start()

        @pl.when(t < tiles - 1)
        def _():
            a_s[:, pl.ds(pl.multiple_of(t * wide, HEAD), wide)] = acc

        @pl.when(t == tiles - 1)
        def _():
            a_s[:, (tiles - 1) * wide : width] = acc[:, over:]

        return 0

    lax.fori_loop(0, tiles, sum_tile, 0)
    for c in put(tiles - 1, wide - over):
        c.start()
    for t in range(tiles - 1):
        for c in put(t):
            c.wait()
    for c in put(tiles - 1, wide - over):
        c.wait()
    for c in outs:
        c.wait()


def chunk(x, gain, cs, wq, wk, wv, wo, w_sib, ks, vs, at, rows, split):
    d, cols = wq.shape
    heads, n = cols // HEAD, len(ks)
    keys, half = at + rows, d // 2
    sib = jax.ShapeDtypeStruct((cols, half), BF)
    got = pl.pallas_call(
        functools.partial(_chunk, at=at, n=n, n_sums=split),
        in_specs=[HBM, pl.BlockSpec((d,), lambda: (0,)), pl.BlockSpec((rows, HEAD), lambda: (0, 0)), HBM, HBM, HBM, HBM] + [HBM] * (2 * n + (n > 0)),
        out_specs=[HBM] * (2 + split + (n == 0)),
        out_shape=[sib] * (n == 0) + [jax.ShapeDtypeStruct((rows // split, half), BF)] * split + [jax.ShapeDtypeStruct((heads, rows, HEAD), BF)] * 2,
        scratch_shapes=[pltpu.VMEM((4, 64, d), BF), pltpu.VMEM((rows, d), BF), pltpu.VMEM((SLOTS, d, 512), BF), pltpu.VMEM((3 * heads + 1, rows, HEAD), BF),
                        pltpu.VMEM((rows, 2 * cols), BF), pltpu.VMEM((keys, rows), jnp.float32), pltpu.VMEM((keys, rows), jnp.float32), pltpu.VMEM((16, rows), jnp.float32), pltpu.VMEM((rows, 512), BF)]
        + [pltpu.VMEM(k.shape, BF) for k in (*ks, *vs)]
        + [pltpu.SemaphoreType.DMA((4,)), pltpu.SemaphoreType.DMA((SLOTS,)), pltpu.SemaphoreType.DMA((max(2 * n, 1),)), pltpu.SemaphoreType.DMA((2,)),
           pltpu.SemaphoreType.DMA((2 * SLOTS, 2)), pltpu.SemaphoreType.DMA((half // 512 + 1, split)), pltpu.SemaphoreType.DMA((heads // 2 + 1,)), pltpu.SemaphoreType.DMA((heads // 2 + 1,)),
           pltpu.SemaphoreType.DMA((7,)), pltpu.SemaphoreType.DMA((7,))],
        compiler_params=pltpu.CompilerParams(vmem_limit_bytes=VM, collective_id=n, has_side_effects=True),
        cost_estimate=pl.CostEstimate(flops=2 * rows * d * (3 * cols + 2 * cols) + 4 * rows * keys * cols, transcendentals=heads * rows * keys,
                                      bytes_accessed=2 * (5 * d * cols + rows * d + 3 * rows * cols + 2 * keys * cols)),
        name="chunk",
    )(x, gain, cs[at : at + rows], wq, wk, wv, wo, *ks, *vs, *([] if n == 0 else [w_sib]))
    got = got if n == 0 else (w_sib, *got)
    return got[0], got[1:-2], got[-2], got[-1]


def _finish(half_ref, x_ref, own, sib, rown, rsib, *ys):
    y_ref = ys[-1]
    n = own.shape[1]
    for c in range(2):
        @pl.when(half_ref[0] == c)
        def _():
            def few(i, _):
                r = pl.ds(pl.multiple_of(i * 16, 16), 16)
                for cols, s, o in ((pl.ds(c * n, n), own, rown), (pl.ds((1 - c) * n, n), sib, rsib)):
                    y_ref[r, cols] = (x_ref[r, cols].astype(jnp.float32) + (s[r, :].astype(jnp.float32) + o[r, :].astype(jnp.float32))).astype(BF)
                return 0

            lax.fori_loop(0, y_ref.shape[0] // 16, few, 0)


def finish(half, x, own, sib, rown, rsib, y, at):
    rows, n = own.shape
    bm = 128
    wide = pl.BlockSpec((bm, 2 * n), lambda t, h: (at // bm + t, 0))
    part = pl.BlockSpec((bm, n), lambda t, h: (t, 0))
    return pl.pallas_call(
        _finish,
        grid_spec=pltpu.PrefetchScalarGridSpec(num_scalar_prefetch=1, grid=(rows // bm,), in_specs=[wide, part, part, part, part] + [HBM] * len(y), out_specs=wide),
        out_shape=jax.ShapeDtypeStruct(x.shape, BF),
        input_output_aliases={6: 0} if y else {},
        compiler_params=pltpu.CompilerParams(dimension_semantics=("arbitrary",)),
        cost_estimate=pl.CostEstimate(flops=rows * n * 2000, bytes_accessed=rows * n * 2 * 8, transcendentals=0),
        name="finish",
    )(half, x, own, sib, rown, rsib, *y)


def tables(rows):
    angle = np.arange(rows, dtype=np.float32)[:, None] * (10000.0 ** (-np.arange(64, dtype=np.float32) / 64)).astype(np.float32)
    return np.concatenate([np.cos(angle), np.sin(angle)], 1).astype(np.float32)


SIB = [(0, 1), (1, 0), (2, 3), (3, 2)]
CROSS = [(0, 2), (2, 0), (1, 3), (3, 1)]
CHUNKS = ((384, 1), (512, 1), (512, 1), (384, 1), (256, 2))


def solution(mesh):
    def step(x, gain, wq, wk, wv, wo):
        cs = jnp.asarray(tables(x.shape[0]))
        half = (lax.axis_index("tp") % 2).astype(jnp.int32)[None]
        ks, vs, sums = [], [], []
        w_sib, at = None, 0
        for rows, split in CHUNKS:
            w_sib, owns, k, v = chunk(x, gain, cs, wq, wk, wv, wo, w_sib, ks, vs, at, rows, split)
            ks.append(k)
            vs.append(v)
            gain, owns = lax.optimization_barrier((gain, owns))
            for own in owns:
                rown = lax.ppermute(own, "tp", CROSS)
                sib = lax.ppermute(own, "tp", SIB)
                rsib = lax.ppermute(rown, "tp", SIB)
                sums.append((own, sib, rown, rsib, at))
                at += rows // split
        y = ()
        for own, sib, rown, rsib, at in sums:
            y = (finish(half, x, own, sib, rown, rsib, y, at),)
        return y[0]

    tokens, columns = P("dp", None), P(None, "tp")
    return jax.shard_map(step, mesh=mesh, in_specs=(tokens, P(None), columns, columns, columns, P("tp", None)), out_specs=tokens, check_vma=False)
```
